256 devices in a mesh: depth: 64 (over x, z, core), tile: 4 (over y).
Axes of the slice: x: 4, y: 4, z: 8, core: 2. Of those that a mesh axis runs over, the one named last changes fastest.
Arguments:
- brick_image: float32 [64, 4, 512, 512], P('depth', None, 'tile'), may hold values from 0 to 0.08
- order: int32 [64], replicated, may hold values from 0 to 63, each once
- active: int32 [64, 4], replicated, may hold values 0 or 1
Outputs:
- final_image: float32 [4, 512, 512], replicated
The draws below stay inside these ranges and needn't reach their ends.
All inputs are finite; a program needn't handle non-finite values.
Results may differ from the reference program's by a relative error of at most 0.00002.
Values sent between devices are 32-bit elements; how exact they have to be, the bound alone decides.
A program may use at most 64 MiB of HBM per device.

```python
import jax
import jax.numpy as jnp
from jax import lax

TILE_ROWS = 128
COLS = 512
ROWS = 512
RANKS = 64
N_TILE = 4


def with_ends(drawn, key, low, top_value):
    dims = drawn.shape
    spot = [jax.random.randint(jax.random.fold_in(key, axis), (), 0, dims[axis]) for axis in range(len(dims))]
    drawn = drawn.at[tuple(spot)].set(low)
    longest = dims.index(max(dims))
    spot[longest] = (spot[longest] + 1) % dims[longest]
    return drawn.at[tuple(spot)].set(top_value)


def level_of(rng, extent, shards, smallest, top_value):
    def one(dim, parts):
        draws = jax.random.uniform(jax.random.fold_in(jax.random.fold_in(rng, 6), dim), (parts,), jnp.float32, smallest / len(shards), top_value / len(shards))
        return jnp.repeat(jnp.exp(draws), extent[dim] // parts).reshape((-1,) + (1,) * (len(extent) - dim - 1))

    level = one(*shards[0])
    for cut in shards[1:]:
        level = level * one(*cut)
    return level


def setup_inputs(seed: int = 0) -> dict:
    arg_keys = jax.random.split(jax.random.key(seed), 4)
    brick_image = jnp.clip(0.08 * jax.random.uniform(arg_keys[0], (RANKS, 4, ROWS, COLS), jnp.float32) ** level_of(arg_keys[0], (RANKS, 4, ROWS, COLS), ((0, 64), (2, 4)), -0.2, 0.2), 0.0, 0.08)
    order = jax.random.permutation(arg_keys[1], RANKS).astype(jnp.int32)
    active = with_ends((jax.random.randint(arg_keys[2], (RANKS, N_TILE), 0, 4) < 3).astype(jnp.int32), jax.random.fold_in(arg_keys[2], 1), 0, 1)
    return dict(brick_image=brick_image, order=order, active=active)


def reference(brick_image, order, active):
    row_flag = jnp.repeat(active.astype(jnp.float32), TILE_ROWS, axis=1)
    masked = brick_image * row_flag[:, None, :, None]
    ordered = masked[order]

    def blend_layer(accumulated, current):
        return accumulated + (1.0 - accumulated[3:4]) * current, None

    final_image, unused = lax.scan(blend_layer, jnp.zeros(brick_image.shape[1:], jnp.float32), ordered)
    return final_image
```

```python
import jax
import jax.numpy as jnp
from jax import lax
from jax.experimental import pallas as pl
from jax.experimental.pallas import tpu as pltpu
from jax.sharding import Mesh
from jax.sharding import PartitionSpec as P

AXES = ("x", "z", "c", "y")
SIZES = {"x": 4, "z": 8, "c": 2, "y": 4}
DEPTH = ("x", "z", "c")
MESH = pl.DeviceIdType.MESH
ALPHA = 3
CHANNELS = (3, 0, 1, 2)
ROUTES = (0, 0, 0, 1)
PEERS = tuple(
    (dx, dz, dc)
    for dz in (4, 3, 5, 2, 6, 1, 7, 0)
    for dx in (2, 1, 3, 0)
    for dc in (1, 0)
    if dx or dz or dc
)


def shifted(me, **offsets):
    place = dict(me)
    for name, step in offsets.items():
        place[name] = lax.rem(me[name] + step, SIZES[name])
    return place


def target(place):
    return tuple(place[name] for name in AXES)


def wait_bytes(ref, sem):
    pltpu.make_async_copy(ref, ref, sem).wait()


def kernel(
    brick, order, active, out,
    mine, layers_0, layers_1, layers_2, layers_3, weights, order_s, active_s,
    local_sem, a2a_send, a2a_recv, z_send, z_recv, first_send, first_recv, last_send, last_recv, pair_send, pair_recv,
):
    me = {name: lax.axis_index(name) for name in AXES}
    x, z, c, y = (me[name] for name in AXES)
    layers = (layers_0, layers_1, layers_2, layers_3)
    rank = (x * 8 + z) * 2 + c

    barrier = pltpu.get_barrier_semaphore()
    greeted = [shifted(me, x=dx, z=dz, c=dc) for dx, dz, dc in PEERS]
    greeted += [shifted(me, y=dy) for dy in (1, 2, 3)]
    for place in greeted:
        pl.semaphore_signal(barrier, inc=1, device_id=target(place), device_id_type=MESH)

    def tile_of(place):
        row = 64 * place["c"] + 16 * place["x"] + 8 * (place["z"] // 4)
        return pl.ds(pl.multiple_of(row, 8), 8), pl.ds(pl.multiple_of(128 * (place["z"] % 4), 128), 128)

    own_rows, own_columns = tile_of(me)
    local = [
        pltpu.make_async_copy(brick.at[0], mine, local_sem.at[0]),
        pltpu.make_async_copy(order, order_s, local_sem.at[1]),
        pltpu.make_async_copy(active, active_s, local_sem.at[2]),
    ] + [
        pltpu.make_async_copy(brick.at[0, ch, own_rows, own_columns], layers[ch].at[rank], local_sem.at[3 + ch])
        for ch in CHANNELS
    ]
    for copy in local:
        copy.start()
    for copy in local:
        copy.wait()
    pl.semaphore_wait(barrier, len(greeted))

    def send(source, destination, send_sem, recv_sem, place):
        pltpu.make_async_remote_copy(
            src_ref=source, dst_ref=destination, send_sem=send_sem, recv_sem=recv_sem,
            device_id=target(place), device_id_type=MESH,
        ).start()

    def exchange(ch):
        for dx, dz, dc in PEERS:
            place = shifted(me, x=dx, z=dz, c=dc)
            rows, columns = tile_of(place)
            send(mine.at[ch, rows, columns], layers[ch].at[rank], a2a_send.at[ch], a2a_recv.at[ch], place)

    half = z // 4
    inner_rows = pl.ds(pl.multiple_of(8 * half, 8), 8)

    def composite(ch):
        wait_bytes(layers[ch].at[pl.ds(0, 63)], a2a_recv.at[ch])
        if ch == ALPHA:

            def step(k, total):
                brick_index = order_s[k]
                flag = active_s[y, brick_index].astype(jnp.float32)
                weight = (1.0 - total) * flag
                weights[k] = weight
                return total + weight * layers[ALPHA][brick_index]

            total = lax.fori_loop(0, 64, step, jnp.zeros((8, 128), jnp.float32), unroll=8)
        else:

            def step(k, total):
                return total + weights[k] * layers[ch][order_s[k]]

            total = lax.fori_loop(0, 64, step, jnp.zeros((8, 128), jnp.float32), unroll=8)
        out[ch, y, c, x, inner_rows, own_columns] = total
        piece = out.at[ch, y, c, x, inner_rows, own_columns]
        for dz in (4, 3, 5, 2, 6, 1, 7):
            send(piece, piece, z_send, z_recv.at[ch], shifted(me, z=dz))

    def route(ch):
        return c * ROUTES[ch]

    def along(ch, leg, step):
        s = route(ch)
        if leg == 0:
            return shifted(me, x=(1 - s) * step, y=s * step)
        return shifted(me, x=s * step, y=(1 - s) * step)

    def block(ch, back):
        s = route(ch)
        by = lax.rem(y + s * (4 - back), 4)
        bx = lax.rem(x + (1 - s) * (4 - back), 4)
        return out.at[ch, by, c, bx]

    def first(ch):
        wait_bytes(layers[ch].at[pl.ds(0, 7)], z_recv.at[ch])
        piece = block(ch, 0)
        for step in (2, 1, 3):
            send(piece, piece, first_send, first_recv.at[ch, step - 1], along(ch, 0, step))
        for step in (2, 1, 3):
            send(piece, piece, last_send, last_recv.at[ch], along(ch, 1, step))

    def last(ch):
        for back in (1, 3, 2):
            piece = block(ch, back)
            wait_bytes(piece, first_recv.at[ch, back - 1])
            for step in (2, 1, 3):
                send(piece, piece, last_send, last_recv.at[ch], along(ch, 1, step))

    def pair(ch):
        wait_bytes(out.at[ch, pl.ds(0, 3), 0], last_recv.at[ch])
        piece = out.at[ch, :, c]
        send(piece, piece, pair_send, pair_recv.at[ch], shifted(me, c=1))

    a, r, g, b = CHANNELS
    exchange(a)
    exchange(r)
    composite(a)
    exchange(g)
    composite(r)
    first(a)
    exchange(b)
    last(a)
    composite(g)
    first(r)
    last(r)
    pair(a)
    composite(b)
    first(g)
    last(g)
    pair(r)
    first(b)
    last(b)
    pair(g)
    pair(b)
    for ch in CHANNELS:
        wait_bytes(out.at[ch, :, 0], pair_recv.at[ch])
        wait_bytes(layers[ch].at[pl.ds(0, 63)], a2a_send.at[ch])
    wait_bytes(layers[0].at[pl.ds(0, 28)], z_send)
    wait_bytes(out.at[:, 0, 0, pl.ds(0, 3)], first_send)
    wait_bytes(out.at[:, pl.ds(0, 3), 0], last_send)
    wait_bytes(out.at[:, :, 0], pair_send)


def composed(brick_image, order, active):
    dma = pltpu.SemaphoreType.DMA
    image = pl.pallas_call(
        kernel,
        out_shape=jax.ShapeDtypeStruct((4, 4, 2, 4, 16, 512), jnp.float32),
        in_specs=[pl.BlockSpec(memory_space=pl.ANY)] * 3,
        out_specs=pl.BlockSpec(memory_space=pltpu.VMEM),
        scratch_shapes=[
            pltpu.VMEM((4, 128, 512), jnp.float32),
            *[pltpu.VMEM((64, 8, 128), jnp.float32)] * 5,
            pltpu.SMEM((64,), jnp.int32),
            pltpu.SMEM((4, 64), jnp.int32),
            dma((7,)),
            dma((4,)), dma((4,)),
            dma, dma((4,)),
            dma, dma((4, 3)),
            dma, dma((4,)),
            dma, dma((4,)),
        ],
        compiler_params=pltpu.CompilerParams(collective_id=0, has_side_effects=True, vmem_limit_bytes=16 * 2**20),
    )(*(pltpu.with_memory_space_constraint(a, pltpu.HBM) for a in (brick_image, order, active.T)))
    return image.reshape(4, 512, 512)


def solution(mesh):
    split = Mesh(mesh.devices.reshape(4, 8, 2, 4), AXES)
    return jax.shard_map(
        composed,
        mesh=split,
        in_specs=(P(DEPTH, None, "y", None), P(), P()),
        out_specs=P(),
        check_vma=False,
    )
```

```python
import jax
import jax.numpy as jnp
from jax import lax
from jax.experimental import pallas as pl
from jax.experimental.pallas import tpu as pltpu
from jax.sharding import Mesh
from jax.sharding import PartitionSpec as P

AXES = ("x", "z", "c", "y")
SIZES = {"x": 4, "z": 8, "c": 2, "y": 4}
DEPTH = ("x", "z", "c")
MESH = pl.DeviceIdType.MESH
ALPHA = 3
CHANNELS = (3, 0, 1, 2)
ROUTES = (1, 1, 1, 1)
PEERS = tuple(
    (dx, dz, dc)
    for dz in (4, 3, 5, 2, 6, 1, 7, 0)
    for dx in (2, 1, 3, 0)
    for dc in (1, 0)
    if dx or dz or dc
)


def shifted(me, **offsets):
    place = dict(me)
    for name, step in offsets.items():
        place[name] = lax.rem(me[name] + step, SIZES[name])
    return place


def target(place):
    return tuple(place[name] for name in AXES)


def wait_bytes(ref, sem):
    pltpu.make_async_copy(ref, ref, sem).wait()


def kernel(
    brick, order, active, out,
    mine, layers_0, layers_1, layers_2, layers_3, weights, order_s, active_s,
    local_sem, a2a_send, a2a_recv, z_send, z_recv, first_send, first_recv, last_send, last_recv, pair_send, pair_recv,
):
    me = {name: lax.axis_index(name) for name in AXES}
    x, z, c, y = (me[name] for name in AXES)
    layers = (layers_0, layers_1, layers_2, layers_3)
    rank = (x * 8 + z) * 2 + c

    barrier = pltpu.get_barrier_semaphore()
    greeted = [shifted(me, x=dx, z=dz, c=dc) for dx, dz, dc in PEERS]
    greeted += [shifted(me, y=dy) for dy in (1, 2, 3)]
    for place in greeted:
        pl.semaphore_signal(barrier, inc=1, device_id=target(place), device_id_type=MESH)

    def tile_of(place):
        row = 64 * place["c"] + 16 * place["x"] + 8 * (place["z"] // 4)
        return pl.ds(pl.multiple_of(row, 8), 8), pl.ds(pl.multiple_of(128 * (place["z"] % 4), 128), 128)

    own_rows, own_columns = tile_of(me)
    local = [
        pltpu.make_async_copy(brick.at[0], mine, local_sem.at[0]),
        pltpu.make_async_copy(order, order_s, local_sem.at[1]),
        pltpu.make_async_copy(active, active_s, local_sem.at[2]),
    ] + [
        pltpu.make_async_copy(brick.at[0, ch, own_rows, own_columns], layers[ch].at[rank], local_sem.at[3 + ch])
        for ch in CHANNELS
    ]
    for copy in local:
        copy.start()
    for copy in local:
        copy.wait()
    pl.semaphore_wait(barrier, len(greeted))

    def send(source, destination, send_sem, recv_sem, place):
        pltpu.make_async_remote_copy(
            src_ref=source, dst_ref=destination, send_sem=send_sem, recv_sem=recv_sem,
            device_id=target(place), device_id_type=MESH,
        ).start()

    def exchange(ch):
        for dx, dz, dc in PEERS:
            place = shifted(me, x=dx, z=dz, c=dc)
            rows, columns = tile_of(place)
            send(mine.at[ch, rows, columns], layers[ch].at[rank], a2a_send.at[ch], a2a_recv.at[ch], place)

    half = z // 4
    inner_rows = pl.ds(pl.multiple_of(8 * half, 8), 8)

    def composite(ch):
        wait_bytes(layers[ch].at[pl.ds(0, 63)], a2a_recv.at[ch])
        if ch == ALPHA:

            def step(k, total):
                brick_index = order_s[k]
                flag = active_s[y, brick_index].astype(jnp.float32)
                weight = (1.0 - total) * flag
                weights[k] = weight
                return total + weight * layers[ALPHA][brick_index]

            total = lax.fori_loop(0, 64, step, jnp.zeros((8, 128), jnp.float32), unroll=8)
        else:

            def step(k, total):
                return total + weights[k] * layers[ch][order_s[k]]

            total = lax.fori_loop(0, 64, step, jnp.zeros((8, 128), jnp.float32), unroll=8)
        out[ch, y, c, x, inner_rows, own_columns] = total
        piece = out.at[ch, y, c, x, inner_rows, own_columns]
        for dz in (4, 3, 5, 2, 6, 1, 7):
            send(piece, piece, z_send, z_recv.at[ch], shifted(me, z=dz))

    def route(ch):
        return c * ROUTES[ch]

    def along(ch, leg, step):
        s = route(ch)
        if leg == 0:
            return shifted(me, x=(1 - s) * step, y=s * step)
        return shifted(me, x=s * step, y=(1 - s) * step)

    def block(ch, back):
        s = route(ch)
        by = lax.rem(y + s * (4 - back), 4)
        bx = lax.rem(x + (1 - s) * (4 - back), 4)
        return out.at[ch, by, c, bx]

    def first(ch):
        wait_bytes(layers[ch].at[pl.ds(0, 7)], z_recv.at[ch])
        piece = block(ch, 0)
        for step in (2, 1, 3):
            send(piece, piece, first_send, first_recv.at[ch, step - 1], along(ch, 0, step))
        for step in (2, 1, 3):
            send(piece, piece, last_send, last_recv.at[ch], along(ch, 1, step))

    def last(ch):
        for back in (1, 3, 2):
            piece = block(ch, back)
            wait_bytes(piece, first_recv.at[ch, back - 1])
            for step in (2, 1, 3):
                send(piece, piece, last_send, last_recv.at[ch], along(ch, 1, step))

    def pair(ch):
        wait_bytes(out.at[ch, pl.ds(0, 3), 0], last_recv.at[ch])
        piece = out.at[ch, :, c]
        send(piece, piece, pair_send, pair_recv.at[ch], shifted(me, c=1))

    a, r, g, b = CHANNELS
    exchange(a)
    exchange(r)
    composite(a)
    exchange(g)
    composite(r)
    first(a)
    exchange(b)
    last(a)
    composite(g)
    first(r)
    last(r)
    pair(a)
    composite(b)
    first(g)
    last(g)
    pair(r)
    first(b)
    last(b)
    pair(g)
    pair(b)
    for ch in CHANNELS:
        wait_bytes(out.at[ch, :, 0], pair_recv.at[ch])
        wait_bytes(layers[ch].at[pl.ds(0, 63)], a2a_send.at[ch])
    wait_bytes(layers[0].at[pl.ds(0, 28)], z_send)
    wait_bytes(out.at[:, 0, 0, pl.ds(0, 3)], first_send)
    wait_bytes(out.at[:, pl.ds(0, 3), 0], last_send)
    wait_bytes(out.at[:, :, 0], pair_send)


def composed(brick_image, order, active):
    dma = pltpu.SemaphoreType.DMA
    image = pl.pallas_call(
        kernel,
        out_shape=jax.ShapeDtypeStruct((4, 4, 2, 4, 16, 512), jnp.float32),
        in_specs=[pl.BlockSpec(memory_space=pl.ANY)] * 3,
        out_specs=pl.BlockSpec(memory_space=pltpu.VMEM),
        scratch_shapes=[
            pltpu.VMEM((4, 128, 512), jnp.float32),
            *[pltpu.VMEM((64, 8, 128), jnp.float32)] * 5,
            pltpu.SMEM((64,), jnp.int32),
            pltpu.SMEM((4, 64), jnp.int32),
            dma((7,)),
            dma((4,)), dma((4,)),
            dma, dma((4,)),
            dma, dma((4, 3)),
            dma, dma((4,)),
            dma, dma((4,)),
        ],
        compiler_params=pltpu.CompilerParams(collective_id=0, has_side_effects=True, vmem_limit_bytes=16 * 2**20),
    )(*(pltpu.with_memory_space_constraint(a, pltpu.HBM) for a in (brick_image, order, active.T)))
    return image.reshape(4, 512, 512)


def solution(mesh):
    split = Mesh(mesh.devices.reshape(4, 8, 2, 4), AXES)
    return jax.shard_map(
        composed,
        mesh=split,
        in_specs=(P(DEPTH, None, "y", None), P(), P()),
        out_specs=P(),
        check_vma=False,
    )
```

```python
import jax
import jax.numpy as jnp
from jax import lax
from jax.experimental import pallas as pl
from jax.experimental.pallas import tpu as pltpu
from jax.sharding import Mesh
from jax.sharding import PartitionSpec as P

AXES = ("x", "z", "c", "y")
SIZES = {"x": 4, "z": 8, "c": 2, "y": 4}
DEPTH = ("x", "z", "c")
MESH = pl.DeviceIdType.MESH
ALPHA = 3
CHANNELS = (3, 0, 1, 2)
UNITS = {"a": (3, 0, 8), "r": (0, 0, 8), "g": (1, 0, 8), "b": (2, 0, 4), "d": (2, 4, 2), "e": (2, 6, 2)}
NAMES = tuple(UNITS)
DIRECT = "e"
FAR_STEP = (0, 1, 2, 1)
FIELD = tuple(
    sorted(((dx, dy) for dx in range(4) for dy in range(4) if dx or dy), key=lambda step: -FAR_STEP[step[0]] - FAR_STEP[step[1]])
)
SCHEDULE = "ea er ca eg cr eb ed fa la cg ee fr cb fg lr cd fb ce lg fd lb de pa pr ld pg pb pd we"
PEERS = tuple(
    (dx, dz, dc)
    for dz in (4, 3, 5, 2, 6, 1, 7, 0)
    for dx in (2, 1, 3, 0)
    for dc in (1, 0)
    if dx or dz or dc
)


def shifted(me, **offsets):
    place = dict(me)
    for name, step in offsets.items():
        place[name] = lax.rem(me[name] + step, SIZES[name])
    return place


def target(place):
    return tuple(place[name] for name in AXES)


def wait_bytes(ref, sem):
    pltpu.make_async_copy(ref, ref, sem).wait()


def kernel(
    brick, order, active, out,
    mine, layers_a, layers_r, layers_g, layers_b, layers_d, layers_e, weights, order_s, active_s,
    ruler, local_sem, send_sem, a2a_recv, z_recv, first_recv, last_recv, pair_recv, field_recv,
):
    me = {name: lax.axis_index(name) for name in AXES}
    x, z, c, y = (me[name] for name in AXES)
    layers = (layers_a, layers_r, layers_g, layers_b, layers_d, layers_e)
    rank = (x * 8 + z) * 2 + c

    def tile_of(place):
        row = 64 * place["c"] + 16 * place["x"] + 8 * (place["z"] // 4)
        return pl.multiple_of(row, 8), pl.ds(pl.multiple_of(128 * (place["z"] % 4), 128), 128)

    own_row, own_columns = tile_of(me)
    def local(source, destination, k):
        return pltpu.make_async_copy(source, destination, local_sem.at[k])

    moved = [local(brick.at[0, ch], mine.at[ch], int(ch != ALPHA)) for ch in CHANNELS]
    rest = moved[1:] + [local(order, order_s, 3), local(active, active_s, 4)]
    for u, (ch, top, rows) in enumerate(UNITS.values()):
        own = brick.at[0, ch, pl.ds(pl.multiple_of(own_row + top, rows), rows), own_columns]
        rest.append(local(own, layers[u].at[rank], 2))
    moved[0].start()
    barrier = pltpu.get_barrier_semaphore()
    greeted = [shifted(me, x=dx, z=dz, c=dc) for dx, dz, dc in PEERS]
    greeted += [shifted(me, y=dy) for dy in (1, 2, 3)]
    for place in greeted:
        pl.semaphore_signal(barrier, inc=1, device_id=target(place), device_id_type=MESH)
    for copy in rest:
        copy.start()
    pl.semaphore_wait(barrier, len(greeted))

    def send(source, destination, recv_sem, place):
        pltpu.make_async_remote_copy(
            src_ref=source, dst_ref=destination, send_sem=send_sem, recv_sem=recv_sem,
            device_id=target(place), device_id_type=MESH,
        ).start()

    def exchange(u):
        ch, top, rows = UNITS[NAMES[u]]
        for dx, dz, dc in PEERS:
            place = shifted(me, x=dx, z=dz, c=dc)
            row, columns = tile_of(place)
            piece = mine.at[ch, pl.ds(pl.multiple_of(row + top, rows), rows), columns]
            send(piece, layers[u].at[rank], a2a_recv.at[u], place)

    half = z // 4

    def composite(u):
        ch, top, rows = UNITS[NAMES[u]]
        wait_bytes(layers[u].at[pl.ds(0, 63)], a2a_recv.at[u])
        if ch == ALPHA:

            def step(k, total):
                brick_index = order_s[k]
                flag = active_s[y, brick_index].astype(jnp.float32)
                weight = (1.0 - total) * flag
                weights[k] = weight
                return total + weight * layers[u][brick_index]

        else:

            def step(k, total):
                return total + weights[k, pl.ds(top, rows)] * layers[u][order_s[k]]

        total = lax.fori_loop(0, 64, step, jnp.zeros((rows, 128), jnp.float32), unroll=8)
        out[ch, y, c, x, half, pl.ds(top, rows), own_columns] = total
        piece = out.at[ch, y, c, x, half, pl.ds(top, rows), own_columns]
        for dz in (4, 3, 5, 2, 6, 1, 7):
            send(piece, piece, z_recv.at[u], shifted(me, z=dz))

    def along(leg, step):
        on_x = c if leg else 1 - c
        return shifted(me, x=on_x * step, y=(1 - on_x) * step)

    def block(u, back, over=0):
        ch, top, rows = UNITS[NAMES[u]]
        by = lax.rem(y + c * (4 - back) + (1 - c) * (4 - over), 4)
        bx = lax.rem(x + (1 - c) * (4 - back) + c * (4 - over), 4)
        return out.at[ch, by, c, bx, :, pl.ds(top, rows)]

    partner = shifted(me, c=1)

    def share(u, over):
        for back in range(4):
            piece = block(u, back, over)
            send(piece, piece, pair_recv, partner)

    def first(u):
        wait_bytes(layers[u].at[pl.ds(0, 7)], z_recv.at[u])
        piece = block(u, 0)
        for step in (2, 1, 3):
            send(piece, piece, first_recv.at[u, step - 1], along(0, step))
        for step in (2, 1, 3):
            send(piece, piece, last_recv.at[u, step - 1], along(1, step))

    def last(u):
        for back in (1, 3, 2):
            piece = block(u, back)
            wait_bytes(piece, first_recv.at[u, back - 1])
            for step in (2, 1, 3):
                send(piece, piece, last_recv.at[u, step - 1], along(1, step))
        share(u, 0)

    def direct(u):
        wait_bytes(layers[u].at[pl.ds(0, 7)], z_recv.at[u])
        piece = block(u, 0)
        for dx, dy in FIELD:
            send(piece, piece, field_recv.at[FAR_STEP[dx] + FAR_STEP[dy] - 1], shifted(me, x=dx, y=dy))
        send(piece, piece, pair_recv, partner)

    def finish(u):
        ch, top, rows = UNITS[NAMES[u]]
        for hops in (1, 2, 3, 4):
            ahead = [step for step in FIELD if FAR_STEP[step[0]] + FAR_STEP[step[1]] == hops]
            wait_bytes(whole(u, 0, 0, pl.ds(0, 4)) if len(ahead) == 4 else whole(u, 0, 0, pl.ds(0, 1)) if len(ahead) == 1 else whole(u, pl.ds(0, 2), 0, pl.ds(0, 3)), field_recv.at[hops - 1])
            for dx, dy in ahead:
                piece = out.at[ch, lax.rem(y + 4 - dy, 4), c, lax.rem(x + 4 - dx, 4), :, pl.ds(top, rows)]
                send(piece, piece, pair_recv, partner)

    def whole(u, *place):
        ch, top, rows = UNITS[NAMES[u]]
        return out.at[ch, *place, :, pl.ds(top, rows)]

    def pair(u):
        for step in (1, 3, 2):
            wait_bytes(whole(u, 0, 0, pl.ds(0, 4)), last_recv.at[u, step - 1])
            share(u, step)

    def ready(u):
        if u == 0:
            wait_bytes(mine.at[ALPHA], local_sem.at[0])
        if u == 1:
            wait_bytes(mine.at[pl.ds(0, 3)], local_sem.at[1])
        exchange(u)

    steps = dict(d=direct, w=finish, e=ready, c=composite, f=first, l=last, p=pair)
    for name in SCHEDULE.split():
        if name == "ca":
            wait_bytes(layers[0].at[pl.ds(0, 4)], local_sem.at[2])
            rest[3].wait()
            rest[4].wait()
        steps[name[0]](NAMES.index(name[1]))
    wait_bytes(out.at[:, :, 0], pair_recv)
    wait_bytes(ruler, send_sem)


def composed(brick_image, order, active):
    dma, count = pltpu.SemaphoreType.DMA, len(UNITS)
    image = pl.pallas_call(
        kernel,
        out_shape=jax.ShapeDtypeStruct((4, 4, 2, 4, 2, 8, 512), jnp.float32),
        in_specs=[pl.BlockSpec(memory_space=pl.ANY)] * 3,
        out_specs=pl.BlockSpec(memory_space=pltpu.VMEM),
        scratch_shapes=[
            pltpu.VMEM((4, 128, 512), jnp.float32),
            *[pltpu.VMEM((64, rows, 128), jnp.float32) for _, _, rows in UNITS.values()],
            pltpu.VMEM((64, 8, 128), jnp.float32),
            pltpu.SMEM((64,), jnp.int32),
            pltpu.SMEM((4, 64), jnp.int32),
            pltpu.VMEM((1272, 8, 128), jnp.float32),
            dma((5,)),
            dma,
            dma((count,)),
            dma((count,)),
            dma((count - 1, 3)),
            dma((count - 1, 3)),
            dma,
            dma((4,)),
        ],
        compiler_params=pltpu.CompilerParams(collective_id=0, has_side_effects=True, vmem_limit_bytes=16 * 2**20),
    )(*(pltpu.with_memory_space_constraint(a, pltpu.HBM) for a in (brick_image, order, active.T)))
    return image.reshape(4, 512, 512)


def solution(mesh):
    split = Mesh(mesh.devices.reshape(4, 8, 2, 4), AXES)
    return jax.shard_map(
        composed,
        mesh=split,
        in_specs=(P(DEPTH, None, "y", None), P(), P()),
        out_specs=P(),
        check_vma=False,
    )
```

```python
import jax
import jax.numpy as jnp
from jax import lax
from jax.experimental import pallas as pl
from jax.experimental.pallas import tpu as pltpu
from jax.sharding import Mesh
from jax.sharding import PartitionSpec as P

AXES = ("x", "z", "c", "y")
SIZES = {"x": 4, "z": 8, "c": 2, "y": 4}
DEPTH = ("x", "z", "c")
MESH = pl.DeviceIdType.MESH
ALPHA = 3
CHANNELS = (3, 0, 1, 2)
UNITS = {"a": (3, 0, 8), "r": (0, 0, 8), "g": (1, 0, 8), "b": (2, 0, 4), "d": (2, 4, 2), "e": (2, 6, 2)}
NAMES = tuple(UNITS)
DIRECT = "e"
HEAD = 40
FAR_STEP = (0, 1, 2, 1)
FIELD = tuple(
    sorted(((dx, dy) for dx in range(4) for dy in range(4) if dx or dy), key=lambda step: -FAR_STEP[step[0]] - FAR_STEP[step[1]])
)
SCHEDULE = (
    "ea", "er", "ca", "hg", "cr", "tg", "eb", "ed", "fa", "fr", "la", "cg",
    "ee", "cb", "lr", "fg", "cd", "fb", "ce", "lg", "fd", "lb", "de", "pa",
    "pr", "ld", "pg", "pb", "pd", "we",
)
PEERS = tuple(
    (dx, dz, dc)
    for dz in (4, 3, 5, 2, 6, 1, 7, 0)
    for dx in (2, 1, 3, 0)
    for dc in (1, 0)
    if dx or dz or dc
)


def shifted(me, **offsets):
    place = dict(me)
    for name, step in offsets.items():
        place[name] = lax.rem(me[name] + step, SIZES[name])
    return place


def target(place):
    return tuple(place[name] for name in AXES)


def wait_bytes(ref, sem):
    pltpu.make_async_copy(ref, ref, sem).wait()


def kernel(
    brick, order, active, out,
    mine, layers_a, layers_r, layers_g, layers_b, layers_d, layers_e, weights, order_s, active_s,
    ruler, local_sem, send_sem, a2a_recv, z_recv, first_recv, last_recv, pair_recv, field_recv,
):
    me = {name: lax.axis_index(name) for name in AXES}
    x, z, c, y = (me[name] for name in AXES)
    layers = (layers_a, layers_r, layers_g, layers_b, layers_d, layers_e)
    rank = (x * 8 + z) * 2 + c

    def tile_of(place):
        row = 64 * place["c"] + 16 * place["x"] + 8 * (place["z"] // 4)
        return pl.multiple_of(row, 8), pl.ds(pl.multiple_of(128 * (place["z"] % 4), 128), 128)

    own_row, own_columns = tile_of(me)
    def local(source, destination, k):
        return pltpu.make_async_copy(source, destination, local_sem.at[k])

    moved = [local(brick.at[0, ch], mine.at[ch], int(ch != ALPHA)) for ch in CHANNELS]
    rest = moved[1:] + [local(order, order_s, 3), local(active, active_s, 4)]
    for u, (ch, top, rows) in enumerate(UNITS.values()):
        own = brick.at[0, ch, pl.ds(pl.multiple_of(own_row + top, rows), rows), own_columns]
        rest.append(local(own, layers[u].at[rank], 2))
    moved[0].start()
    barrier = pltpu.get_barrier_semaphore()
    greeted = [shifted(me, x=dx, z=dz, c=dc) for dx, dz, dc in PEERS]
    greeted += [shifted(me, y=dy) for dy in (1, 2, 3)]
    for place in greeted:
        pl.semaphore_signal(barrier, inc=1, device_id=target(place), device_id_type=MESH)
    for copy in rest:
        copy.start()
    pl.semaphore_wait(barrier, len(greeted))

    def send(source, destination, recv_sem, place):
        pltpu.make_async_remote_copy(
            src_ref=source, dst_ref=destination, send_sem=send_sem, recv_sem=recv_sem,
            device_id=target(place), device_id_type=MESH,
        ).start()

    def exchange(u, peers=PEERS):
        ch, top, rows = UNITS[NAMES[u]]
        for dx, dz, dc in peers:
            place = shifted(me, x=dx, z=dz, c=dc)
            row, columns = tile_of(place)
            piece = mine.at[ch, pl.ds(pl.multiple_of(row + top, rows), rows), columns]
            send(piece, layers[u].at[rank], a2a_recv.at[u], place)

    half = z // 4

    def composite(u):
        ch, top, rows = UNITS[NAMES[u]]
        wait_bytes(layers[u].at[pl.ds(0, 63)], a2a_recv.at[u])
        if ch == ALPHA:

            def step(k, total):
                brick_index = order_s[k]
                flag = active_s[y, brick_index].astype(jnp.float32)
                weight = (1.0 - total) * flag
                weights[k] = weight
                return total + weight * layers[u][brick_index]

        else:

            def step(k, total):
                return total + weights[k, pl.ds(top, rows)] * layers[u][order_s[k]]

        total = lax.fori_loop(0, 64, step, jnp.zeros((rows, 128), jnp.float32), unroll=8)
        out[ch, y, c, x, half, pl.ds(top, rows), own_columns] = total
        piece = out.at[ch, y, c, x, half, pl.ds(top, rows), own_columns]
        for dz in (4, 3, 5, 2, 6, 1, 7):
            send(piece, piece, z_recv.at[u], shifted(me, z=dz))

    def along(leg, step):
        on_x = c if leg else 1 - c
        return shifted(me, x=on_x * step, y=(1 - on_x) * step)

    def block(u, back, over=0):
        ch, top, rows = UNITS[NAMES[u]]
        by = lax.rem(y + c * (4 - back) + (1 - c) * (4 - over), 4)
        bx = lax.rem(x + (1 - c) * (4 - back) + c * (4 - over), 4)
        return out.at[ch, by, c, bx, :, pl.ds(top, rows)]

    partner = shifted(me, c=1)

    def share(u, over):
        for back in range(4):
            piece = block(u, back, over)
            send(piece, piece, pair_recv, partner)

    def first(u):
        wait_bytes(layers[u].at[pl.ds(0, 7)], z_recv.at[u])
        piece = block(u, 0)
        for step in (2, 1, 3):
            send(piece, piece, first_recv.at[u, step - 1], along(0, step))
        for step in (2, 1, 3):
            send(piece, piece, last_recv.at[u, step - 1], along(1, step))

    def last(u):
        for back in (1, 3, 2):
            piece = block(u, back)
            wait_bytes(piece, first_recv.at[u, back - 1])
            for step in (2, 1, 3):
                send(piece, piece, last_recv.at[u, step - 1], along(1, step))
        share(u, 0)

    def direct(u):
        wait_bytes(layers[u].at[pl.ds(0, 7)], z_recv.at[u])
        piece = block(u, 0)
        for dx, dy in FIELD:
            send(piece, piece, field_recv.at[FAR_STEP[dx] + FAR_STEP[dy] - 1], shifted(me, x=dx, y=dy))
        send(piece, piece, pair_recv, partner)

    def finish(u):
        ch, top, rows = UNITS[NAMES[u]]
        for hops in (1, 2, 3, 4):
            ahead = [step for step in FIELD if FAR_STEP[step[0]] + FAR_STEP[step[1]] == hops]
            wait_bytes(whole(u, 0, 0, pl.ds(0, 4)) if len(ahead) == 4 else whole(u, 0, 0, pl.ds(0, 1)) if len(ahead) == 1 else whole(u, pl.ds(0, 2), 0, pl.ds(0, 3)), field_recv.at[hops - 1])
            for dx, dy in ahead:
                piece = out.at[ch, lax.rem(y + 4 - dy, 4), c, lax.rem(x + 4 - dx, 4), :, pl.ds(top, rows)]
                send(piece, piece, pair_recv, partner)

    def whole(u, *place):
        ch, top, rows = UNITS[NAMES[u]]
        return out.at[ch, *place, :, pl.ds(top, rows)]

    def pair(u):
        for step in (1, 3, 2):
            wait_bytes(whole(u, 0, 0, pl.ds(0, 4)), last_recv.at[u, step - 1])
            share(u, step)

    def ready(u):
        if u == 0:
            wait_bytes(mine.at[ALPHA], local_sem.at[0])
        if u == 1:
            wait_bytes(mine.at[pl.ds(0, 3)], local_sem.at[1])
        exchange(u)

    def head(u):
        exchange(u, PEERS[:HEAD])

    def tail(u):
        exchange(u, PEERS[HEAD:])

    steps = dict(h=head, t=tail, d=direct, w=finish, e=ready, c=composite, f=first, l=last, p=pair)
    for name in SCHEDULE:
        if name == "ca":
            wait_bytes(layers[0].at[pl.ds(0, 4)], local_sem.at[2])
            rest[3].wait()
            rest[4].wait()
        steps[name[0]](NAMES.index(name[1]))
    wait_bytes(out.at[:, :, 0], pair_recv)
    wait_bytes(ruler, send_sem)


def composed(brick_image, order, active):
    dma, count = pltpu.SemaphoreType.DMA, len(UNITS)
    image = pl.pallas_call(
        kernel,
        out_shape=jax.ShapeDtypeStruct((4, 4, 2, 4, 2, 8, 512), jnp.float32),
        in_specs=[pl.BlockSpec(memory_space=pl.ANY)] * 3,
        out_specs=pl.BlockSpec(memory_space=pltpu.VMEM),
        scratch_shapes=[
            pltpu.VMEM((4, 128, 512), jnp.float32),
            *[pltpu.VMEM((64, rows, 128), jnp.float32) for _, _, rows in UNITS.values()],
            pltpu.VMEM((64, 8, 128), jnp.float32),
            pltpu.SMEM((64,), jnp.int32),
            pltpu.SMEM((4, 64), jnp.int32),
            pltpu.VMEM((1272, 8, 128), jnp.float32),
            dma((5,)),
            dma,
            dma((count,)),
            dma((count,)),
            dma((count - 1, 3)),
            dma((count - 1, 3)),
            dma,
            dma((4,)),
        ],
        compiler_params=pltpu.CompilerParams(collective_id=0, has_side_effects=True, vmem_limit_bytes=16 * 2**20),
    )(*(pltpu.with_memory_space_constraint(a, pltpu.HBM) for a in (brick_image, order, active.T)))
    return image.reshape(4, 512, 512)


def solution(mesh):
    split = Mesh(mesh.devices.reshape(4, 8, 2, 4), AXES)
    return jax.shard_map(
        composed,
        mesh=split,
        in_specs=(P(DEPTH, None, "y", None), P(), P()),
        out_specs=P(),
        check_vma=False,
    )
```

```python
import jax
import jax.numpy as jnp
from jax import lax
from jax.experimental import pallas as pl
from jax.experimental.pallas import tpu as pltpu
from jax.sharding import Mesh
from jax.sharding import PartitionSpec as P

AXES = ("x", "z", "c", "y")
SIZES = {"x": 4, "z": 8, "c": 2, "y": 4}
DEPTH = ("x", "z", "c")
MESH = pl.DeviceIdType.MESH
ALPHA = 3
CHANNELS = (3, 0, 1, 2)
UNITS = {"a": (3, 0, 8), "r": (0, 0, 8), "g": (1, 0, 8), "b": (2, 0, 4), "d": (2, 4, 2), "e": (2, 6, 2)}
NAMES = tuple(UNITS)
DIRECT = "e"
HEAD = 40
FAR_STEP = (0, 1, 2, 1)
FIELD = tuple(
    sorted(((dx, dy) for dx in range(4) for dy in range(4) if dx or dy), key=lambda step: -FAR_STEP[step[0]] - FAR_STEP[step[1]])
)
SCHEDULE = (
    "ea", "er", "ca", "hg", "cr", "tg", "eb", "ed", "fa", "fr", "la", "cg",
    "ee", "cb", "lr", "fg", "cd", "ce", "fb", "lg", "fd", "de", "lb", "pa",
    "pr", "ld", "pg", "pb", "pd", "we",
)
PEERS = tuple(
    (dx, dz, dc)
    for dz in (4, 3, 5, 2, 6, 1, 7, 0)
    for dx in (2, 1, 3, 0)
    for dc in (1, 0)
    if dx or dz or dc
)


def shifted(me, **offsets):
    place = dict(me)
    for name, step in offsets.items():
        place[name] = lax.rem(me[name] + step, SIZES[name])
    return place


def target(place):
    return tuple(place[name] for name in AXES)


def wait_bytes(ref, sem):
    pltpu.make_async_copy(ref, ref, sem).wait()


def kernel(
    brick, order, active, out,
    mine, layers_a, layers_r, layers_g, layers_b, layers_d, layers_e, weights, order_s, active_s,
    ruler, local_sem, send_sem, a2a_recv, z_recv, first_recv, last_recv, pair_recv, field_recv,
):
    me = {name: lax.axis_index(name) for name in AXES}
    x, z, c, y = (me[name] for name in AXES)
    layers = (layers_a, layers_r, layers_g, layers_b, layers_d, layers_e)
    rank = (x * 8 + z) * 2 + c

    def tile_of(place):
        row = 64 * place["c"] + 16 * place["x"] + 8 * (place["z"] // 4)
        return pl.multiple_of(row, 8), pl.ds(pl.multiple_of(128 * (place["z"] % 4), 128), 128)

    own_row, own_columns = tile_of(me)
    def local(source, destination, k):
        return pltpu.make_async_copy(source, destination, local_sem.at[k])

    moved = [local(brick.at[0, ch], mine.at[ch], int(ch != ALPHA)) for ch in CHANNELS]
    rest = moved[1:] + [local(order, order_s, 3), local(active, active_s, 4)]
    for u, (ch, top, rows) in enumerate(UNITS.values()):
        own = brick.at[0, ch, pl.ds(pl.multiple_of(own_row + top, rows), rows), own_columns]
        rest.append(local(own, layers[u].at[rank], 2))
    moved[0].start()
    barrier = pltpu.get_barrier_semaphore()
    greeted = [shifted(me, x=dx, z=dz, c=dc) for dx, dz, dc in PEERS]
    greeted += [shifted(me, y=dy) for dy in (1, 2, 3)]
    for place in greeted:
        pl.semaphore_signal(barrier, inc=1, device_id=target(place), device_id_type=MESH)
    for copy in rest:
        copy.start()
    pl.semaphore_wait(barrier, len(greeted))

    def send(source, destination, recv_sem, place):
        pltpu.make_async_remote_copy(
            src_ref=source, dst_ref=destination, send_sem=send_sem, recv_sem=recv_sem,
            device_id=target(place), device_id_type=MESH,
        ).start()

    def exchange(u, peers=PEERS):
        ch, top, rows = UNITS[NAMES[u]]
        for dx, dz, dc in peers:
            place = shifted(me, x=dx, z=dz, c=dc)
            row, columns = tile_of(place)
            piece = mine.at[ch, pl.ds(pl.multiple_of(row + top, rows), rows), columns]
            send(piece, layers[u].at[rank], a2a_recv.at[u], place)

    half = z // 4

    def composite(u):
        ch, top, rows = UNITS[NAMES[u]]
        wait_bytes(layers[u].at[pl.ds(0, 63)], a2a_recv.at[u])
        if ch == ALPHA:

            def step(k, total):
                brick_index = order_s[k]
                flag = active_s[y, brick_index].astype(jnp.float32)
                weight = (1.0 - total) * flag
                weights[k] = weight
                return total + weight * layers[u][brick_index]

        else:

            def step(k, total):
                return total + weights[k, pl.ds(top, rows)] * layers[u][order_s[k]]

        total = lax.fori_loop(0, 64, step, jnp.zeros((rows, 128), jnp.float32), unroll=8)
        out[ch, y, c, x, half, pl.ds(top, rows), own_columns] = total
        piece = out.at[ch, y, c, x, half, pl.ds(top, rows), own_columns]
        for dz in (4, 3, 5, 2, 6, 1, 7):
            send(piece, piece, z_recv.at[u], shifted(me, z=dz))

    def along(leg, step):
        on_x = c if leg else 1 - c
        return shifted(me, x=on_x * step, y=(1 - on_x) * step)

    def block(u, back, over=0):
        ch, top, rows = UNITS[NAMES[u]]
        by = lax.rem(y + c * (4 - back) + (1 - c) * (4 - over), 4)
        bx = lax.rem(x + (1 - c) * (4 - back) + c * (4 - over), 4)
        return out.at[ch, by, c, bx, :, pl.ds(top, rows)]

    partner = shifted(me, c=1)

    def share(u, over):
        for back in range(4):
            piece = block(u, back, over)
            send(piece, piece, pair_recv, partner)

    def first(u):
        wait_bytes(layers[u].at[pl.ds(0, 7)], z_recv.at[u])
        piece = block(u, 0)
        for step in (2, 1, 3):
            send(piece, piece, first_recv.at[u, step - 1], along(0, step))
        for step in (2, 1, 3):
            send(piece, piece, last_recv.at[u, step - 1], along(1, step))

    def last(u):
        for back in (1, 3, 2):
            piece = block(u, back)
            wait_bytes(piece, first_recv.at[u, back - 1])
            for step in (2, 1, 3):
                send(piece, piece, last_recv.at[u, step - 1], along(1, step))
        share(u, 0)

    def direct(u):
        wait_bytes(layers[u].at[pl.ds(0, 7)], z_recv.at[u])
        piece = block(u, 0)
        for dx, dy in FIELD:
            send(piece, piece, field_recv.at[FAR_STEP[dx] + FAR_STEP[dy] - 1], shifted(me, x=dx, y=dy))
        send(piece, piece, pair_recv, partner)

    def finish(u):
        ch, top, rows = UNITS[NAMES[u]]
        for hops in (1, 2, 3, 4):
            ahead = [step for step in FIELD if FAR_STEP[step[0]] + FAR_STEP[step[1]] == hops]
            wait_bytes(whole(u, 0, 0, pl.ds(0, 4)) if len(ahead) == 4 else whole(u, 0, 0, pl.ds(0, 1)) if len(ahead) == 1 else whole(u, pl.ds(0, 2), 0, pl.ds(0, 3)), field_recv.at[hops - 1])
            for dx, dy in ahead:
                piece = out.at[ch, lax.rem(y + 4 - dy, 4), c, lax.rem(x + 4 - dx, 4), :, pl.ds(top, rows)]
                send(piece, piece, pair_recv, partner)

    def whole(u, *place):
        ch, top, rows = UNITS[NAMES[u]]
        return out.at[ch, *place, :, pl.ds(top, rows)]

    def pair(u):
        for step in (1, 3, 2):
            wait_bytes(whole(u, 0, 0, pl.ds(0, 4)), last_recv.at[u, step - 1])
            share(u, step)

    def ready(u):
        if u == 0:
            wait_bytes(mine.at[ALPHA], local_sem.at[0])
        if u == 1:
            wait_bytes(mine.at[pl.ds(0, 3)], local_sem.at[1])
        exchange(u)

    def head(u):
        exchange(u, PEERS[:HEAD])

    def tail(u):
        exchange(u, PEERS[HEAD:])

    steps = dict(h=head, t=tail, d=direct, w=finish, e=ready, c=composite, f=first, l=last, p=pair)
    for name in SCHEDULE:
        if name == "ca":
            wait_bytes(layers[0].at[pl.ds(0, 4)], local_sem.at[2])
            rest[3].wait()
            rest[4].wait()
        steps[name[0]](NAMES.index(name[1]))
    wait_bytes(out.at[:, :, 0], pair_recv)
    wait_bytes(ruler, send_sem)


def composed(brick_image, order, active):
    dma, count = pltpu.SemaphoreType.DMA, len(UNITS)
    image = pl.pallas_call(
        kernel,
        out_shape=jax.ShapeDtypeStruct((4, 4, 2, 4, 2, 8, 512), jnp.float32),
        in_specs=[pl.BlockSpec(memory_space=pl.ANY)] * 3,
        out_specs=pl.BlockSpec(memory_space=pltpu.VMEM),
        scratch_shapes=[
            pltpu.VMEM((4, 128, 512), jnp.float32),
            *[pltpu.VMEM((64, rows, 128), jnp.float32) for _, _, rows in UNITS.values()],
            pltpu.VMEM((64, 8, 128), jnp.float32),
            pltpu.SMEM((64,), jnp.int32),
            pltpu.SMEM((4, 64), jnp.int32),
            pltpu.VMEM((1272, 8, 128), jnp.float32),
            dma((5,)),
            dma,
            dma((count,)),
            dma((count,)),
            dma((count - 1, 3)),
            dma((count - 1, 3)),
            dma,
            dma((4,)),
        ],
        compiler_params=pltpu.CompilerParams(collective_id=0, has_side_effects=True, vmem_limit_bytes=16 * 2**20),
    )(*(pltpu.with_memory_space_constraint(a, pltpu.HBM) for a in (brick_image, order, active.T)))
    return image.reshape(4, 512, 512)


def solution(mesh):
    split = Mesh(mesh.devices.reshape(4, 8, 2, 4), AXES)
    return jax.shard_map(
        composed,
        mesh=split,
        in_specs=(P(DEPTH, None, "y", None), P(), P()),
        out_specs=P(),
        check_vma=False,
    )
```

```python
import jax
import jax.numpy as jnp
from jax import lax
from jax.experimental import pallas as pl
from jax.experimental.pallas import tpu as pltpu
from jax.sharding import Mesh
from jax.sharding import PartitionSpec as P

AXES = ("x", "z", "c", "y")
SIZES = {"x": 4, "z": 8, "c": 2, "y": 4}
DEPTH = ("x", "z", "c")
MESH = pl.DeviceIdType.MESH
ALPHA = 3
CHANNELS = (3, 0, 1, 2)
UNITS = {"a": (3, 0, 8), "r": (0, 0, 8), "g": (1, 0, 8), "b": (2, 0, 4), "d": (2, 4, 2), "e": (2, 6, 2)}
NAMES = tuple(UNITS)
DIRECT = "e"
HEAD = 40
FAR_STEP = (0, 1, 2, 1)
FIELD = tuple(
    sorted(((dx, dy) for dx in range(4) for dy in range(4) if dx or dy), key=lambda step: -FAR_STEP[step[0]] - FAR_STEP[step[1]])
)
SCHEDULE = (
    "ea", "er", "ca", "hg", "cr", "tg", "eb", "ed", "fa", "fr", "la", "cg",
    "ee", "cb", "lr", "fg", "cd", "ce", "fb", "lg", "fd", "de", "lb", "pa",
    "pr", "ld", "pg", "pb", "pd", "we",
)
PEERS = tuple(
    (dx, dz, dc)
    for dz in (4, 3, 5, 2, 6, 1, 7, 0)
    for dx in (2, 1, 3, 0)
    for dc in (1, 0)
    if dx or dz or dc
)


def shifted(me, **offsets):
    place = dict(me)
    for name, step in offsets.items():
        place[name] = lax.rem(me[name] + step, SIZES[name])
    return place


def target(place):
    return tuple(place[name] for name in AXES)


def wait_bytes(ref, sem):
    pltpu.make_async_copy(ref, ref, sem).wait()


def kernel(
    brick, order, active, out,
    mine, layers_a, layers_r, layers_g, layers_b, layers_d, layers_e, weights, order_s, active_s,
    ruler, local_sem, send_sem, a2a_recv, z_recv, first_recv, last_recv, pair_recv, field_recv,
):
    me = {name: lax.axis_index(name) for name in AXES}
    x, z, c, y = (me[name] for name in AXES)
    layers = (layers_a, layers_r, layers_g, layers_b, layers_d, layers_e)
    rank = (x * 8 + z) * 2 + c

    def tile_of(place):
        row = 64 * place["c"] + 16 * place["x"] + 8 * (place["z"] // 4)
        return pl.multiple_of(row, 8), pl.ds(pl.multiple_of(128 * (place["z"] % 4), 128), 128)

    own_row, own_columns = tile_of(me)
    def local(source, destination, k):
        return pltpu.make_async_copy(source, destination, local_sem.at[k])

    moved = [local(brick.at[0, ch], mine.at[ch], int(ch != ALPHA)) for ch in CHANNELS]
    rest = moved[1:] + [local(order, order_s, 3), local(active, active_s, 4)]
    for u, (ch, top, rows) in enumerate(UNITS.values()):
        own = brick.at[0, ch, pl.ds(pl.multiple_of(own_row + top, rows), rows), own_columns]
        rest.append(local(own, layers[u].at[rank], 2))
    moved[0].start()
    barrier = pltpu.get_barrier_semaphore()
    greeted = [shifted(me, x=dx, z=dz, c=dc) for dx, dz, dc in PEERS]
    greeted += [shifted(me, y=dy) for dy in (1, 2, 3)]
    for place in greeted:
        pl.semaphore_signal(barrier, inc=1, device_id=target(place), device_id_type=MESH)
    for copy in rest:
        copy.start()
    pl.semaphore_wait(barrier, len(greeted))

    def send(source, destination, recv_sem, place):
        pltpu.make_async_remote_copy(
            src_ref=source, dst_ref=destination, send_sem=send_sem, recv_sem=recv_sem,
            device_id=target(place), device_id_type=MESH,
        ).start()

    def exchange(u, peers=PEERS):
        ch, top, rows = UNITS[NAMES[u]]
        for dx, dz, dc in peers:
            place = shifted(me, x=dx, z=dz, c=dc)
            row, columns = tile_of(place)
            piece = mine.at[ch, pl.ds(pl.multiple_of(row + top, rows), rows), columns]
            send(piece, layers[u].at[rank], a2a_recv.at[u], place)

    half = z // 4

    def composite(u):
        ch, top, rows = UNITS[NAMES[u]]
        wait_bytes(layers[u].at[pl.ds(0, 63)], a2a_recv.at[u])
        if ch == ALPHA:

            def step(k, total):
                brick_index = order_s[k]
                flag = active_s[y, brick_index].astype(jnp.float32)
                weight = (1.0 - total) * flag
                weights[k] = weight
                return total + weight * layers[u][brick_index]

        else:

            def step(k, total):
                return total + weights[k, pl.ds(top, rows)] * layers[u][order_s[k]]

        total = lax.fori_loop(0, 64, step, jnp.zeros((rows, 128), jnp.float32), unroll=16)
        out[ch, y, c, x, half, pl.ds(top, rows), own_columns] = total
        piece = out.at[ch, y, c, x, half, pl.ds(top, rows), own_columns]
        for dz in (4, 3, 5, 2, 6, 1, 7):
            send(piece, piece, z_recv.at[u], shifted(me, z=dz))

    def along(leg, step):
        on_x = c if leg else 1 - c
        return shifted(me, x=on_x * step, y=(1 - on_x) * step)

    def block(u, back, over=0):
        ch, top, rows = UNITS[NAMES[u]]
        by = lax.rem(y + c * (4 - back) + (1 - c) * (4 - over), 4)
        bx = lax.rem(x + (1 - c) * (4 - back) + c * (4 - over), 4)
        return out.at[ch, by, c, bx, :, pl.ds(top, rows)]

    partner = shifted(me, c=1)

    def share(u, over):
        for back in range(4):
            piece = block(u, back, over)
            send(piece, piece, pair_recv, partner)

    def first(u):
        wait_bytes(layers[u].at[pl.ds(0, 7)], z_recv.at[u])
        piece = block(u, 0)
        for step in (2, 1, 3):
            send(piece, piece, first_recv.at[u, step - 1], along(0, step))
        for step in (2, 1, 3):
            send(piece, piece, last_recv.at[u, step - 1], along(1, step))

    def last(u):
        for back in (1, 3, 2):
            piece = block(u, back)
            wait_bytes(piece, first_recv.at[u, back - 1])
            for step in (2, 1, 3):
                send(piece, piece, last_recv.at[u, step - 1], along(1, step))
        share(u, 0)

    def direct(u):
        wait_bytes(layers[u].at[pl.ds(0, 7)], z_recv.at[u])
        piece = block(u, 0)
        for dx, dy in FIELD:
            send(piece, piece, field_recv.at[FAR_STEP[dx] + FAR_STEP[dy] - 1], shifted(me, x=dx, y=dy))
        send(piece, piece, pair_recv, partner)

    def finish(u):
        ch, top, rows = UNITS[NAMES[u]]
        for hops in (1, 2, 3, 4):
            ahead = [step for step in FIELD if FAR_STEP[step[0]] + FAR_STEP[step[1]] == hops]
            wait_bytes(whole(u, 0, 0, pl.ds(0, 4)) if len(ahead) == 4 else whole(u, 0, 0, pl.ds(0, 1)) if len(ahead) == 1 else whole(u, pl.ds(0, 2), 0, pl.ds(0, 3)), field_recv.at[hops - 1])
            for dx, dy in ahead:
                piece = out.at[ch, lax.rem(y + 4 - dy, 4), c, lax.rem(x + 4 - dx, 4), :, pl.ds(top, rows)]
                send(piece, piece, pair_recv, partner)

    def whole(u, *place):
        ch, top, rows = UNITS[NAMES[u]]
        return out.at[ch, *place, :, pl.ds(top, rows)]

    def pair(u):
        for step in (1, 3, 2):
            wait_bytes(whole(u, 0, 0, pl.ds(0, 4)), last_recv.at[u, step - 1])
            share(u, step)

    def ready(u):
        if u == 0:
            wait_bytes(mine.at[ALPHA], local_sem.at[0])
        if u == 1:
            wait_bytes(mine.at[pl.ds(0, 3)], local_sem.at[1])
        exchange(u)

    def head(u):
        exchange(u, PEERS[:HEAD])

    def tail(u):
        exchange(u, PEERS[HEAD:])

    steps = dict(h=head, t=tail, d=direct, w=finish, e=ready, c=composite, f=first, l=last, p=pair)
    for name in SCHEDULE:
        if name == "ca":
            wait_bytes(layers[0].at[pl.ds(0, 4)], local_sem.at[2])
            rest[3].wait()
            rest[4].wait()
        steps[name[0]](NAMES.index(name[1]))
    wait_bytes(out.at[:, :, 0], pair_recv)
    wait_bytes(ruler, send_sem)


def composed(brick_image, order, active):
    dma, count = pltpu.SemaphoreType.DMA, len(UNITS)
    image = pl.pallas_call(
        kernel,
        out_shape=jax.ShapeDtypeStruct((4, 4, 2, 4, 2, 8, 512), jnp.float32),
        in_specs=[pl.BlockSpec(memory_space=pl.ANY)] * 3,
        out_specs=pl.BlockSpec(memory_space=pltpu.VMEM),
        scratch_shapes=[
            pltpu.VMEM((4, 128, 512), jnp.float32),
            *[pltpu.VMEM((64, rows, 128), jnp.float32) for _, _, rows in UNITS.values()],
            pltpu.VMEM((64, 8, 128), jnp.float32),
            pltpu.SMEM((64,), jnp.int32),
            pltpu.SMEM((4, 64), jnp.int32),
            pltpu.VMEM((1272, 8, 128), jnp.float32),
            dma((5,)),
            dma,
            dma((count,)),
            dma((count,)),
            dma((count - 1, 3)),
            dma((count - 1, 3)),
            dma,
            dma((4,)),
        ],
        compiler_params=pltpu.CompilerParams(collective_id=0, has_side_effects=True, vmem_limit_bytes=16 * 2**20),
    )(*(pltpu.with_memory_space_constraint(a, pltpu.HBM) for a in (brick_image, order, active.T)))
    return image.reshape(4, 512, 512)


def solution(mesh):
    split = Mesh(mesh.devices.reshape(4, 8, 2, 4), AXES)
    return jax.shard_map(
        composed,
        mesh=split,
        in_specs=(P(DEPTH, None, "y", None), P(), P()),
        out_specs=P(),
        check_vma=False,
    )
```
